32 devices in a mesh: dp: 4 (over y, z), ep: 8 (over x, core).
Axes of the slice: x: 4, y: 2, z: 2, core: 2. Of those that a mesh axis runs over, the one named last changes fastest.
The devices are a block of a 4x4x8 slice.
Arguments:
- x_tokens: bfloat16 [16384, 2048], P(('dp', 'ep')), parts along dimension 0
- dy_tokens: bfloat16 [16384, 2048], P(('dp', 'ep')), parts along dimension 0
- expert_ids: int32 [16384, 10], P(('dp', 'ep')), parts along dimension 0
- gate_vals: float32 [16384, 10], P(('dp', 'ep')), parts along dimension 0
- slot_pos: int32 [16384, 10], P(('dp', 'ep')), parts along dimension 0
- w_gate: bfloat16 [16, 2048, 512], P('ep')
- w_up: bfloat16 [16, 2048, 512], P('ep')
- w_down: bfloat16 [16, 512, 2048], P('ep')
- shared_gate: bfloat16 [2048, 512], replicated
- shared_up: bfloat16 [2048, 512], replicated
- shared_down: bfloat16 [512, 2048], replicated
Outputs:
- output 1: bfloat16 [16384, 2048], P(('dp', 'ep')), parts along dimension 0
- output 2: float32 [64, 2048, 512], P(('dp', 'ep')), parts along dimension 0
- output 3: float32 [64, 2048, 512], P(('dp', 'ep')), parts along dimension 0
- output 4: float32 [64, 512, 2048], P(('dp', 'ep')), parts along dimension 0
- output 5: float32 [32, 2048, 512], P(('dp', 'ep')), parts along dimension 0
- output 6: float32 [32, 2048, 512], P(('dp', 'ep')), parts along dimension 0
- output 7: float32 [32, 512, 2048], P(('dp', 'ep')), parts along dimension 0
There are 4 independent parts. The reference program is written for one: setup_inputs(seed, part) draws one part's arguments, and reference() takes and returns one part's arrays. A program takes and returns all parts, laid end to end along the dimension named above; an argument that names none is the same for every part.
All inputs are finite; a program needn't handle non-finite values.
Results may differ from the reference program's by a relative error of at most 0.00172.
Values are sent between devices in bfloat16 or wider.
A program may use at most 768 MiB of HBM per device.

```python
import jax
import jax.numpy as jnp
from jax import lax

MODEL_DIM = 2048
EXPERT_FF = 512
SHARED_FF = 512
TOP_K = 10
TOK_DEV = 512
GROUP_SIZE = 8
NUM_EXPERTS = 16
CAPACITY = 480


def draw_routing(route_key):
    bias_key, hot_key, noise_key = jax.random.split(route_key, 3)
    expert_range = jnp.arange(NUM_EXPERTS, dtype=jnp.int32)
    expert_bias = jax.random.randint(bias_key, (NUM_EXPERTS,), 0, 256)
    hot_expert = jax.random.randint(hot_key, (GROUP_SIZE,), 0, NUM_EXPERTS)
    noise = jax.random.randint(noise_key, (GROUP_SIZE, TOK_DEV, NUM_EXPERTS), 0, 1024)
    forced = (jnp.arange(TOK_DEV)[None, :, None] < CAPACITY) & (expert_range[None, None, :] == hot_expert[:, None, None])
    score = (noise + expert_bias[None, None, :] + 4096 * forced.astype(jnp.int32)) * NUM_EXPERTS + expert_range
    choices = lax.top_k(score, TOP_K)[1]

    def source_slots(source_choices):
        flat_choices = source_choices.reshape(-1)
        onehot = (flat_choices[:, None] == expert_range[None, :]).astype(jnp.int32)
        earlier = jnp.cumsum(onehot, axis=0) - onehot
        slot_rank = jnp.sum(earlier * onehot, axis=1)
        return jnp.where(slot_rank < CAPACITY, slot_rank, -1).reshape(TOK_DEV, TOP_K)

    positions = lax.map(source_slots, choices)
    return choices.reshape(-1, TOP_K).astype(jnp.int32), positions.reshape(-1, TOP_K).astype(jnp.int32)


def setup_inputs(seed: int = 0, part: int = 0) -> dict:
    part_key = jax.random.fold_in(jax.random.key(seed), part)
    key_x, key_dy, key_gate, key_route = jax.random.split(part_key, 4)
    weight_keys = jax.random.split(jax.random.key(seed + 1), 6)
    tokens = GROUP_SIZE * TOK_DEV
    x_tokens = jax.random.normal(key_x, (tokens, MODEL_DIM), jnp.float32).astype(jnp.bfloat16)
    dy_tokens = jax.random.normal(key_dy, (tokens, MODEL_DIM), jnp.float32).astype(jnp.bfloat16)
    gate_vals = jax.random.uniform(key_gate, (tokens, TOP_K), jnp.float32, 0.25, 1.0)
    expert_ids, slot_pos = draw_routing(key_route)
    in_scale = MODEL_DIM ** -0.5
    ff_scale = EXPERT_FF ** -0.5
    shared_scale = SHARED_FF ** -0.5
    w_gate = (jax.random.normal(weight_keys[0], (NUM_EXPERTS, MODEL_DIM, EXPERT_FF), jnp.float32) * in_scale).astype(jnp.bfloat16)
    w_up = (jax.random.normal(weight_keys[1], (NUM_EXPERTS, MODEL_DIM, EXPERT_FF), jnp.float32) * in_scale).astype(jnp.bfloat16)
    w_down = (jax.random.normal(weight_keys[2], (NUM_EXPERTS, EXPERT_FF, MODEL_DIM), jnp.float32) * ff_scale).astype(jnp.bfloat16)
    shared_gate = (jax.random.normal(weight_keys[3], (MODEL_DIM, SHARED_FF), jnp.float32) * in_scale).astype(jnp.bfloat16)
    shared_up = (jax.random.normal(weight_keys[4], (MODEL_DIM, SHARED_FF), jnp.float32) * in_scale).astype(jnp.bfloat16)
    shared_down = (jax.random.normal(weight_keys[5], (SHARED_FF, MODEL_DIM), jnp.float32) * shared_scale).astype(jnp.bfloat16)
    return {'x_tokens': x_tokens, 'dy_tokens': dy_tokens, 'expert_ids': expert_ids, 'gate_vals': gate_vals, 'slot_pos': slot_pos, 'w_gate': w_gate, 'w_up': w_up, 'w_down': w_down, 'shared_gate': shared_gate, 'shared_up': shared_up, 'shared_down': shared_down}


def expert_grads(x_rows, dz_rows, gate_w, up_w, down_w):
    act_gate = jnp.dot(x_rows, gate_w, preferred_element_type=jnp.float32).astype(jnp.bfloat16)
    act_up = jnp.dot(x_rows, up_w, preferred_element_type=jnp.float32).astype(jnp.bfloat16)
    gate_f32 = act_gate.astype(jnp.float32)
    up_f32 = act_up.astype(jnp.float32)
    sigma = jax.nn.sigmoid(gate_f32)
    silu_gate = gate_f32 * sigma
    hidden = (silu_gate * up_f32).astype(jnp.bfloat16)
    grad_hidden = jnp.dot(dz_rows, down_w.T, preferred_element_type=jnp.float32)
    grad_gate = (grad_hidden * up_f32 * sigma * (1.0 + gate_f32 * (1.0 - sigma))).astype(jnp.bfloat16)
    grad_up = (grad_hidden * silu_gate).astype(jnp.bfloat16)
    grad_down_w = jnp.dot(hidden.T, dz_rows, preferred_element_type=jnp.float32)
    grad_gate_w = jnp.dot(x_rows.T, grad_gate, preferred_element_type=jnp.float32)
    grad_up_w = jnp.dot(x_rows.T, grad_up, preferred_element_type=jnp.float32)
    grad_rows = jnp.dot(grad_gate, gate_w.T, preferred_element_type=jnp.float32) + jnp.dot(grad_up, up_w.T, preferred_element_type=jnp.float32)
    return grad_rows, grad_gate_w, grad_up_w, grad_down_w


def reference(x_tokens, dy_tokens, expert_ids, gate_vals, slot_pos, w_gate, w_up, w_down, shared_gate, shared_up, shared_down):
    tokens = GROUP_SIZE * TOK_DEV
    slot_rows = GROUP_SIZE * CAPACITY
    total_rows = NUM_EXPERTS * slot_rows
    source = jnp.arange(tokens, dtype=jnp.int32)[:, None] // TOK_DEV
    target = jnp.where(slot_pos >= 0, expert_ids * slot_rows + source * CAPACITY + slot_pos, total_rows).reshape(-1)
    token_index = jnp.broadcast_to(jnp.arange(tokens, dtype=jnp.int32)[:, None], (tokens, TOP_K)).reshape(-1)
    row_token = jnp.full((total_rows + 1,), tokens, jnp.int32).at[target].set(token_index)[:total_rows].reshape(NUM_EXPERTS, slot_rows)
    row_gate = jnp.zeros((total_rows + 1,), jnp.float32).at[target].set(gate_vals.reshape(-1))[:total_rows].reshape(NUM_EXPERTS, slot_rows)

    def expert_step(routed_sum, expert_in):
        token_rows, gate_rows, gate_w, up_w, down_w = expert_in
        x_rows = jnp.take(x_tokens, token_rows, axis=0, mode='fill', fill_value=0)
        dy_rows = jnp.take(dy_tokens, token_rows, axis=0, mode='fill', fill_value=0)
        dz_rows = (dy_rows.astype(jnp.float32) * gate_rows[:, None]).astype(jnp.bfloat16)
        grad_rows, grad_gate_w, grad_up_w, grad_down_w = expert_grads(x_rows, dz_rows, gate_w, up_w, down_w)
        returned = grad_rows.astype(jnp.bfloat16).astype(jnp.float32)
        routed_sum = routed_sum.at[token_rows].add(returned, mode='drop')
        return routed_sum, (grad_gate_w, grad_up_w, grad_down_w)

    routed_sum, expert_w_grads = lax.scan(expert_step, jnp.zeros((tokens, MODEL_DIM), jnp.float32), (row_token, row_gate, w_gate, w_up, w_down))
    grad_w_gate, grad_w_up, grad_w_down = expert_w_grads

    def shared_step(source_in):
        x_rows, dy_rows = source_in
        return expert_grads(x_rows, dy_rows, shared_gate, shared_up, shared_down)

    shared_dx, grad_shared_gate, grad_shared_up, grad_shared_down = lax.map(shared_step, (x_tokens.reshape(GROUP_SIZE, TOK_DEV, MODEL_DIM), dy_tokens.reshape(GROUP_SIZE, TOK_DEV, MODEL_DIM)))
    grad_x = (routed_sum + shared_dx.reshape(tokens, MODEL_DIM)).astype(jnp.bfloat16)
    return (grad_x, grad_w_gate, grad_w_up, grad_w_down, grad_shared_gate, grad_shared_up, grad_shared_down)
```

```python
import jax
import jax.numpy as jnp
from jax import lax
from jax.sharding import PartitionSpec as P

S = 2


def swiglu_parts(act_gate, act_up, grad_hidden):
    gate_f32 = act_gate.astype(jnp.float32)
    up_f32 = act_up.astype(jnp.float32)
    sigma = jax.nn.sigmoid(gate_f32)
    silu_gate = gate_f32 * sigma
    hidden = (silu_gate * up_f32).astype(jnp.bfloat16)
    grad_gate = (grad_hidden * up_f32 * sigma * (1.0 + gate_f32 * (1.0 - sigma))).astype(jnp.bfloat16)
    grad_up = (grad_hidden * silu_gate).astype(jnp.bfloat16)
    return hidden, grad_gate, grad_up


def dot(spec, a, b):
    return jnp.einsum(spec, a, b, preferred_element_type=jnp.float32)


def shared_backward(x_tokens, dy_tokens, shared_gate, shared_up, shared_down):
    act_gate = dot('td,df->tf', x_tokens, shared_gate).astype(jnp.bfloat16)
    act_up = dot('td,df->tf', x_tokens, shared_up).astype(jnp.bfloat16)
    grad_hidden = dot('td,fd->tf', dy_tokens, shared_down)
    hidden, grad_gate, grad_up = swiglu_parts(act_gate, act_up, grad_hidden)
    grad_gate_w = dot('td,tf->df', x_tokens, grad_gate)
    grad_up_w = dot('td,tf->df', x_tokens, grad_up)
    grad_down_w = dot('tf,td->fd', hidden, dy_tokens)
    grad_input = dot('tf,df->td', grad_gate, shared_gate) + dot('tf,df->td', grad_up, shared_up)
    return grad_input, grad_gate_w, grad_up_w, grad_down_w


def solution(mesh):
    group = mesh.shape['ep']
    token_spec = P(('dp', 'ep'), None)
    expert_spec = P('ep', None, None)
    whole_spec = P(None, None)
    grad_spec = P(('dp', 'ep'), None, None)

    def local_backward(x_tokens, dy_tokens, expert_ids, gate_vals, slot_pos, w_gate, w_up, w_down, shared_gate, shared_up, shared_down):
        tok_count, top_k = expert_ids.shape
        local_experts, model_dim, expert_ff = w_gate.shape
        num_experts = local_experts * group
        step = tok_count // S
        table = jnp.full((tok_count, num_experts), jnp.inf, jnp.float32)
        experts = jnp.arange(num_experts, dtype=jnp.int32)[None, :]
        for j in range(top_k):
            hit = (expert_ids[:, j:j + 1] == experts) & (slot_pos[:, j:j + 1] >= 0)
            table = jnp.where(hit, gate_vals[:, j:j + 1], table)
        table_all = lax.all_gather(table, 'ep')
        mine = lax.dynamic_slice_in_dim(table_all, lax.axis_index('ep') * local_experts, local_experts, axis=2)
        routed = []
        parts = []
        for s in range(S):
            rows = slice(s * step, (s + 1) * step)
            x_all = lax.all_gather(x_tokens[rows], 'ep', tiled=True)
            dy_all = lax.all_gather(dy_tokens[rows], 'ep', tiled=True)
            total = 0.0
            for e in range(local_experts):
                gate = mine[:, rows, e].reshape(-1, 1)
                kept = gate < jnp.inf
                z = (dy_all.astype(jnp.float32) * jnp.where(kept, gate, 0.0)).astype(jnp.bfloat16)
                act_gate = jnp.where(kept, dot('td,df->tf', x_all, w_gate[e]), 0.0).astype(jnp.bfloat16)
                act_up = jnp.where(kept, dot('td,df->tf', x_all, w_up[e]), 0.0).astype(jnp.bfloat16)
                grad_hidden = dot('td,fd->tf', z, w_down[e])
                hidden, grad_gate, grad_up = swiglu_parts(act_gate, act_up, grad_hidden)
                parts.append((e, x_all, z, hidden, grad_gate, grad_up))
                r = dot('tf,df->td', grad_gate, w_gate[e]) + dot('tf,df->td', grad_up, w_up[e])
                total = total + lax.reduce_precision(r, 8, 7)
            routed.append(lax.psum_scatter(total, 'ep', scatter_dimension=0, tiled=True))
        dgs, dus, dds = [], [], []
        for e in range(local_experts):
            dg = du = dd = 0.0
            for (pe, x_all, z, hidden, grad_gate, grad_up) in parts:
                if pe == e:
                    dg = dg + dot('td,tf->df', x_all, grad_gate)
                    du = du + dot('td,tf->df', x_all, grad_up)
                    dd = dd + dot('tf,td->fd', hidden, z)
            dgs.append(dg)
            dus.append(du)
            dds.append(dd)
        routed_sum = jnp.concatenate(routed, axis=0)
        shared_dx, grad_shared_gate, grad_shared_up, grad_shared_down = shared_backward(x_tokens, dy_tokens, shared_gate, shared_up, shared_down)
        grad_x = (routed_sum + shared_dx).astype(jnp.bfloat16)
        return grad_x, jnp.stack(dgs), jnp.stack(dus), jnp.stack(dds), grad_shared_gate[None], grad_shared_up[None], grad_shared_down[None]

    return jax.shard_map(local_backward, mesh=mesh, in_specs=(token_spec, token_spec, token_spec, token_spec, token_spec, expert_spec, expert_spec, expert_spec, whole_spec, whole_spec, whole_spec), out_specs=(token_spec, grad_spec, grad_spec, grad_spec, grad_spec, grad_spec, grad_spec), check_vma=False)
```

```python
import functools

import jax
import jax.numpy as jnp
from jax import lax
from jax.experimental import pallas as pl
from jax.experimental.pallas import tpu as pltpu
from jax.sharding import PartitionSpec as P

CW = 256
F32, BF16 = jnp.float32, jnp.bfloat16
MESH = pl.DeviceIdType.MESH
NN = (((1,), (0,)), ((), ()))
NT = (((1,), (1,)), ((), ()))


def dot(a, b, dims):
    return lax.dot_general(a, b, dims, preferred_element_type=F32)


def moe_kernel(tok, dim, ff, cw, x_loc, dy_loc, gt, w1, w3, w2, s1, s3, s2,
               gx, dw1, dw3, dw2, sw1, sw3, sw2, x_all, dy_all, z_all, pp, q_sum, rsh, from_l, from_r, opp,
               w1v, w3v, w2v, act, xt, dyt, zt, dat, dbt, acc, xc, tmp, gall,
               wsem, gsend, grecv, ssem, rsem, psend, precv, r1s, r1r, r2s, r2r, r3s, r3r, lsem, xcs, o1s, o2s, gxs):
    me = lax.axis_index("ep")
    core = lax.rem(me, 2)
    xpos = me // 2
    right = 2 * lax.rem(xpos + 1, 4) + core
    left = 2 * lax.rem(xpos + 3, 4) + core
    far = 2 * lax.rem(xpos + 2, 4) + core
    mate = 2 * xpos + 1 - core
    half = tok // 2
    rows = tok // 8

    def remote(src, dst, send, recv, dev):
        return pltpu.make_async_remote_copy(src_ref=src, dst_ref=dst, send_sem=send, recv_sem=recv, device_id={"ep": dev}, device_id_type=MESH)

    def local(src, dst, sem):
        return pltpu.make_async_copy(src, dst, sem)

    def o1(b, h):
        return acc.at[b, pl.ds(0, cw), pl.ds((1 + h) * ff, ff)]

    def o2(b, e):
        return acc.at[b, pl.ds(0, ff), pl.ds(e * cw, cw)]

    def load(k, b, s, ref):
        return local(s, ref.at[b], wsem.at[k, b])

    barrier = pltpu.get_barrier_semaphore()
    for d in range(1, 8):
        pl.semaphore_signal(barrier, inc=1, device_id={"ep": lax.rem(me + d, 8)}, device_id_type=MESH)

    shared_loads = [load(0, 1, s1, w1v), load(1, 1, s3, w3v), load(2, 1, s2, w2v)]
    first_loads = [load(0, 0, w1.at[0], w1v), load(1, 0, w3.at[0], w3v), load(2, 0, w2.at[0], w2v)]
    second_loads = [load(0, 1, w1.at[1], w1v), load(1, 1, w3.at[1], w3v), load(2, 1, w2.at[1], w2v)]
    own_loads = [local(x_loc, xt, lsem.at[0]), local(dy_loc, dyt, lsem.at[1])]
    for c in own_loads + shared_loads + first_loads:
        c.start()
    pl.semaphore_wait(barrier, 7)

    def block(ref, slot):
        return ref.at[pl.ds(pl.multiple_of(slot * tok, tok), tok), :]

    gates = []
    for d in range(1, 8):
        peer = lax.rem(me + d, 8)
        gates.append(remote(gt.at[peer], gall.at[me], gsend.at[d], grecv.at[me], peer))
        gates[-1].start()
    own_gate = local(gt.at[me], gall.at[me], lsem.at[2])
    own_gate.start()

    def message(k):
        src_dst = [
            (x_loc, x_all, me, right), (dy_loc, dy_all, me, right), (dy_loc, dy_all, me, left), (x_loc, x_all, me, left),
            (x_loc, x_all, me, mate), (dy_loc, dy_all, me, mate),
            (None, x_all, left, right), (None, dy_all, right, left),
            (None, x_all, left, mate), (None, dy_all, left, mate), (None, x_all, right, mate), (None, dy_all, right, mate),
            (None, x_all, far, mate), (None, dy_all, far, mate),
        ][k]
        src, dst, slot, dev = src_dst
        return remote(block(dst, slot) if src is None else src, block(dst, slot), ssem.at[k], rsem.at[k], dev)

    for k in (4, 5, 0, 2, 1, 3):
        message(k).start()

    def forward(col, wb, ab, routed, gate_row, ab_out, before_sum):
        if routed:
            gate = jnp.transpose(jnp.broadcast_to(gate_row, (128, tok)))
            kept = gate < jnp.inf
            gate = jnp.where(kept, gate, 0.0)
            for n in range(dim // 128):
                s = slice(n * 128, (n + 1) * 128)
                zt[:, s] = (dyt[:, s].astype(F32) * gate).astype(BF16)
            wide = jnp.concatenate([kept] * (cw // 128), axis=1)
            dz = zt
        else:
            dz = dyt
        for n in range(ff // cw):
            s = slice(n * cw, (n + 1) * cw)
            a = dot(xt[...], w1v[wb, :, s], NN)
            b = dot(xt[...], w3v[wb, :, s], NN)
            if routed:
                a = jnp.where(wide, a, 0.0)
                b = jnp.where(wide, b, 0.0)
            a = a.astype(BF16).astype(F32)
            b = b.astype(BF16).astype(F32)
            g = dot(dz[...], w2v[wb, s, :], NT)
            sig = jax.nn.sigmoid(a)
            silu = a * sig
            hid = (silu * b).astype(BF16)
            da = (g * b * sig * (1.0 + a * (1.0 - sig))).astype(BF16)
            db = (g * silu).astype(BF16)
            dat[:, s] = da
            dbt[:, s] = db
            act[ab, 0, s, pl.ds(col, tok)] = jnp.transpose(hid)
            act[ab, 1, s, pl.ds(col, tok)] = jnp.transpose(da)
            act[ab, 2, s, pl.ds(col, tok)] = jnp.transpose(db)
        before_sum()
        for n in range(dim // cw):
            s = slice(n * cw, (n + 1) * cw)
            r = dot(dat[...], w1v[wb, s, :], NT) + dot(dbt[...], w3v[wb, s, :], NT)
            if routed:
                acc[ab_out, :, s] += r.astype(BF16).astype(F32)
            else:
                acc[ab_out, :, s] = r

    for c in own_loads + shared_loads:
        c.wait()
    keep = [local(xt, block(x_all, me), lsem.at[0]), local(dyt, block(dy_all, me), lsem.at[1])]
    for c in keep:
        c.start()
    forward(0, 1, 1, False, None, 1, lambda: None)
    for c in second_loads:
        c.start()
    save = local(acc.at[1], rsh, lsem.at[3])
    save.start()

    def shared_grads(n, _):
        s = pl.ds(pl.multiple_of(n * cw, cw), cw)
        outs = [local(o1(0, 0), sw1.at[s, :], o1s.at[0]), local(o1(0, 1), sw3.at[s, :], o1s.at[1]), local(o2(0, 0), sw2.at[:, s], o2s.at[0])]

        @pl.when(n > 0)
        def _():
            for c in outs:
                c.wait()
        o1(0, 0)[...] = jnp.transpose(dot(act[1, 1, :, 0:tok], xt[:, s], NN))
        o1(0, 1)[...] = jnp.transpose(dot(act[1, 2, :, 0:tok], xt[:, s], NN))
        o2(0, 0)[...] = dot(act[1, 0, :, 0:tok], dyt[:, s], NN)
        for c in outs:
            c.start()
        return 0

    lax.fori_loop(0, dim // cw, shared_grads, 0)
    local(o1(0, 0), sw1.at[pl.ds(0, cw), :], o1s.at[0]).wait()
    local(o1(0, 1), sw3.at[pl.ds(0, cw), :], o1s.at[1]).wait()
    local(o2(0, 0), sw2.at[:, pl.ds(0, cw)], o2s.at[0]).wait()
    save.wait()
    for c in keep + first_loads + second_loads + [own_gate]:
        c.wait()
    for d in range(1, 8):
        peer = lax.rem(me + d, 8)
        remote(gt.at[peer], gall.at[peer], gsend.at[d], grecv.at[peer], peer).wait_recv()

    def phase1(to_left):
        if to_left:
            return remote(q_sum.at[1, pl.ds(0, half), :], from_r.at[pl.ds(0, half), :], r1s.at[0], r1r.at[0], left)
        return remote(q_sum.at[2, pl.ds(half, half), :], from_l.at[pl.ds(half, half), :], r1s.at[1], r1r.at[1], right)

    def phase2(k, to_left):
        if to_left:
            s = pl.ds(half + k * rows, rows)
            return remote(q_sum.at[3, s, :], opp.at[s, :], r2s.at[0, k], r2r.at[0, k], left)
        s = pl.ds(k * rows, rows)
        return remote(q_sum.at[3, s, :], opp.at[s, :], r2s.at[1, k], r2r.at[1, k], right)

    def phase3(k, to_left):
        if to_left:
            s = pl.ds(pl.multiple_of(half + k * rows, rows), rows)
            return remote(acc.at[0, s, :], from_r.at[s, :], r3s.at[0, k], r3r.at[0, k], left)
        s = pl.ds(pl.multiple_of(k * rows, rows), rows)
        return remote(acc.at[0, s, :], from_l.at[s, :], r3s.at[1, k], r3r.at[1, k], right)

    def partial(i):
        return remote(acc.at[0], pp.at[i], psend.at[i], precv.at[i], mate)

    def tile(j, _):
        i = jnp.where(j < 2, 0, jnp.where(j >= 6, 3, 1 + lax.rem(j, 2)))
        t = jnp.where(j < 2, j, jnp.where(j >= 6, j - 6, (j - 2) // 2))
        off = jnp.where(i == 1, 3, jnp.where(i == 2, 1, jnp.where(i == 3, 2, 0)))
        slot = 2 * lax.rem(xpos + off, 4) + jnp.where(t == 0, 1 - core, core)

        @pl.when(j == 0)
        def _():
            message(4).wait_recv()
            message(5).wait_recv()

        @pl.when(j == 2)
        def _():
            for k, outs in ((0, (6, 8)), (2, (7, 11)), (1, (9,)), (3, (10,))):
                message(k).wait_recv()
                for o in outs:
                    message(o).start()
            message(8).wait_recv()
            message(9).wait_recv()

        @pl.when(j == 3)
        def _():
            message(10).wait_recv()
            message(11).wait_recv()

        @pl.when(j == 6)
        def _():
            message(6).wait_recv()
            message(12).start()
            message(7).wait_recv()
            message(13).start()
            message(12).wait_recv()
            message(13).wait_recv()

        loads = [local(block(x_all, slot), xt, lsem.at[0]), local(block(dy_all, slot), dyt, lsem.at[1])]
        for c in loads:
            c.start()
        for c in loads:
            c.wait()
        col = pl.multiple_of(slot * tok, tok)

        def expert(e, _):
            put_z = local(zt, z_all.at[e, pl.ds(col, tok), :], lsem.at[2])

            def before_sum():
                put_z.start()

                @pl.when((e == 0) & (t == 0))
                def _():
                    @pl.when(i > 0)
                    def _():
                        partial(i - 1).wait_send()
                    acc[0] = jnp.zeros((tok, dim), F32)

                @pl.when((e == 0) & (t == 1))
                def _():
                    partial(i).wait_recv()
                    get = local(pp.at[i], acc.at[1], lsem.at[3])
                    get.start()
                    get.wait()

            forward(col, e, e, True, gall[slot, pl.ds(e, 1), :], t, before_sum)
            put_z.wait()
            return 0

        lax.fori_loop(0, 2, expert, 0)

        @pl.when(t == 0)
        def _():
            partial(i).start()

        @pl.when(t == 1)
        def _():
            put = local(acc.at[1], q_sum.at[i], lsem.at[3])
            put.start()
            put.wait()

        @pl.when(j == 4)
        def _():
            phase1(True).start()

        @pl.when(j == 5)
        def _():
            phase1(False).start()

        @pl.when(j == 7)
        def _():
            for k in range(4):
                phase2(k, True).start()
                phase2(k, False).start()
        return 0

    lax.fori_loop(0, 8, tile, 0)
    partial(3).wait_send()

    def combine(k):
        for to_left in (False, True):
            base = half if to_left else 0
            s = pl.ds(pl.multiple_of(base + k * rows, rows), rows)
            b = 0 if to_left else 1
            remote(opp.at[s, :], opp.at[s, :], r2s.at[b, k], r2r.at[b, k], right).wait_recv()
            gets = [local(opp.at[s, :], acc.at[0, s, :], lsem.at[0]), local(q_sum.at[1 if to_left else 2, s, :], tmp.at[0], lsem.at[1])]
            for c in gets:
                c.start()
            for c in gets:
                c.wait()
            acc[0, s, :] += tmp[0]
            phase3(k, to_left).start()

    chunks = dim // cw

    def column(n):
        return pl.ds(pl.multiple_of(n * cw, cw), cw)

    def fetch(kind, n, b):
        src = x_all.at[:, column(n)] if kind == 0 else z_all.at[kind - 1, :, column(n)]
        return local(src, xc.at[b], xcs.at[b])

    fetch(0, 0, 0).start()

    def weight_grads(n, _):
        b0 = lax.rem(3 * n, 2)
        b1 = 1 - b0
        fetch(1, n, b1).start()
        fetch(0, n, b0).wait()
        for e in range(2):
            for h, dst in ((0, dw1), (1, dw3)):
                put = local(o1(1, h), dst.at[e, column(n), :], o1s.at[h])
                if e == 0:
                    @pl.when(n > 0)
                    def _():
                        put.wait()
                else:
                    put.wait()
                o1(1, h)[...] = jnp.transpose(dot(act[e, 1 + h], xc[b0], NN))
                put.start()
        fetch(2, n, b0).start()
        for e in range(2):
            b = b1 if e == 0 else b0
            put = local(o2(1, e), dw2.at[e, :, column(n)], o2s.at[e])
            fetch(1 + e, n, b).wait()
            if e == 1:
                @pl.when(n < chunks - 1)
                def _():
                    fetch(0, n + 1, b1).start()

            @pl.when(n > 0)
            def _():
                put.wait()
            o2(1, e)[...] = dot(act[e, 0], xc[b], NN)
            put.start()

        @pl.when(n >= chunks - 4)
        def _():
            combine(n - (chunks - 4))
        return 0

    lax.fori_loop(0, chunks, weight_grads, 0)

    for h, dst in ((0, dw1), (1, dw3)):
        local(o1(1, h), dst.at[1, column(0), :], o1s.at[h]).wait()
    for e in range(2):
        local(o2(1, e), dw2.at[e, :, column(0)], o2s.at[e]).wait()
    get = local(q_sum.at[0], acc.at[1], lsem.at[2])
    get.start()
    phase1(True).wait_recv()
    phase1(False).wait_recv()
    get.wait()

    def own_rows(k, _):
        s = pl.ds(pl.multiple_of(k * rows, rows), rows)
        first = local(rsh.at[s, :], tmp.at[0], lsem.at[0])
        first.start()

        @pl.when(k < 4)
        def _():
            local(from_r.at[s, :], tmp.at[1], lsem.at[1]).start()

        @pl.when(k >= 4)
        def _():
            local(from_l.at[s, :], tmp.at[1], lsem.at[1]).start()
        first.wait()
        local(from_l.at[s, :], tmp.at[1], lsem.at[1]).wait()
        acc[1, s, :] += tmp[0] + tmp[1]
        return 0

    lax.fori_loop(0, 8, own_rows, 0)

    def last(k):
        sa, sb = pl.ds(k * rows, rows), pl.ds(half + k * rows, rows)
        phase3(k, False).wait_recv()
        ga = local(from_l.at[sa, :], tmp.at[0], lsem.at[0])
        ga.start()
        phase3(k, True).wait_recv()
        gb = local(from_r.at[sb, :], tmp.at[1], lsem.at[1])
        gb.start()
        ga.wait()
        xt[sa, :] = (acc[1, sa, :] + tmp[0]).astype(BF16)
        pa = local(xt.at[sa, :], gx.at[sa, :], gxs.at[0, k])
        pa.start()
        gb.wait()
        xt[sb, :] = (acc[1, sb, :] + tmp[1]).astype(BF16)
        pb = local(xt.at[sb, :], gx.at[sb, :], gxs.at[1, k])
        pb.start()
        return [pa, pb]

    puts = []
    for k in range(4):
        puts += last(k)
    for c in puts:
        c.wait()
    for c in gates:
        c.wait_send()
    for k in range(14):
        message(k).wait_send()
    for to_left in (True, False):
        phase1(to_left).wait_send()
        for k in range(4):
            phase2(k, to_left).wait_send()
            phase3(k, to_left).wait_send()


def moe_call(x, dy, gt, w1, w3, w2, s1, s3, s2):
    tok, dim = x.shape
    ff = w1.shape[2]
    cw = CW
    sds = jax.ShapeDtypeStruct
    outs = [
        sds((tok, dim), BF16), sds((2, dim, ff), F32), sds((2, dim, ff), F32), sds((2, ff, dim), F32),
        sds((dim, ff), F32), sds((dim, ff), F32), sds((ff, dim), F32),
        sds((8 * tok, dim), BF16), sds((8 * tok, dim), BF16), sds((2, 8 * tok, dim), BF16),
        sds((4, tok, dim), F32), sds((4, tok, dim), F32), sds((tok, dim), F32), sds((tok, dim), F32), sds((tok, dim), F32), sds((tok, dim), F32),
    ]
    V, D = pltpu.VMEM, pltpu.SemaphoreType.DMA
    scratch = [
        V((2, dim, ff), BF16), V((2, dim, ff), BF16), V((2, ff, dim), BF16), V((2, 3, ff, 8 * tok), BF16),
        V((tok, dim), BF16), V((tok, dim), BF16), V((tok, dim), BF16), V((tok, ff), BF16), V((tok, ff), BF16),
        V((2, tok, dim), F32), V((2, 8 * tok, cw), BF16), V((2, tok // 8, dim), F32),
        V((8, 8, tok), F32),
        D((3, 2)), D((8,)), D((8,)), D((14,)), D((14,)), D((4,)), D((4,)), D((2,)), D((2,)),
        D((2, 4)), D((2, 4)), D((2, 4)), D((2, 4)), D((4,)), D((2,)), D((2,)), D((2,)), D((2, 4)),
    ]
    any_spec = pl.BlockSpec(memory_space=pl.ANY)
    return pl.pallas_call(
        functools.partial(moe_kernel, tok, dim, ff, cw),
        out_shape=outs,
        in_specs=[any_spec] * 9,
        out_specs=[any_spec] * len(outs),
        scratch_shapes=scratch,
        compiler_params=pltpu.CompilerParams(collective_id=0, has_side_effects=True, vmem_limit_bytes=67043328),
        name="moe_backward",
    )(x, dy, gt, w1, w3, w2, s1, s3, s2)[:7]


def solution(mesh):
    group = mesh.shape['ep']
    token_spec = P(('dp', 'ep'), None)
    expert_spec = P('ep', None, None)
    whole_spec = P(None, None)
    grad_spec = P(('dp', 'ep'), None, None)

    def local_backward(x_tokens, dy_tokens, expert_ids, gate_vals, slot_pos, w_gate, w_up, w_down, shared_gate, shared_up, shared_down):
        tok_count, top_k = expert_ids.shape
        num_experts = w_gate.shape[0] * group
        ids, pos, gates = expert_ids.T, slot_pos.T, gate_vals.T
        experts = jnp.arange(num_experts, dtype=jnp.int32)[:, None]
        table = jnp.full((num_experts, tok_count), jnp.inf, F32)
        for j in range(top_k):
            table = jnp.where((ids[j:j + 1] == experts) & (pos[j:j + 1] >= 0), gates[j:j + 1], table)
        table = jnp.pad(table.reshape(group, -1, tok_count), ((0, 0), (0, 8 - num_experts // group), (0, 0)))
        gx, dw1, dw3, dw2, sw1, sw3, sw2 = moe_call(x_tokens, dy_tokens, table, w_gate, w_up, w_down, shared_gate, shared_up, shared_down)
        return gx, dw1, dw3, dw2, sw1[None], sw3[None], sw2[None]

    return jax.shard_map(local_backward, mesh=mesh, in_specs=(token_spec, token_spec, token_spec, token_spec, token_spec, expert_spec, expert_spec, expert_spec, whole_spec, whole_spec, whole_spec), out_specs=(token_spec, grad_spec, grad_spec, grad_spec, grad_spec, grad_spec, grad_spec), check_vma=False)
```

```python
import functools

import jax
import jax.numpy as jnp
from jax import lax
from jax.experimental import pallas as pl
from jax.experimental.pallas import tpu as pltpu
from jax.sharding import PartitionSpec as P

CW = 256
F32, BF16 = jnp.float32, jnp.bfloat16
MESH = pl.DeviceIdType.MESH
NN = (((1,), (0,)), ((), ()))
NT = (((1,), (1,)), ((), ()))


def dot(a, b, dims):
    return lax.dot_general(a, b, dims, preferred_element_type=F32)


def moe_kernel(tok, dim, ff, cw, x_loc, dy_loc, gt, w1, w3, w2, s1, s3, s2,
               gx, dw1, dw3, dw2, sw1, sw3, sw2, x_all, dy_all, z_all, pp, q_sum, rsh, from_l, from_r, opp,
               w1v, w3v, w2v, act, xt, dyt, zt, dat, dbt, acc, xc, tmp, gall,
               wsem, gsend, grecv, ssem, rsem, psend, precv, r1s, r1r, r2s, r2r, r3s, r3r, lsem, xcs, zcs, o1s, o2s, gxs):
    me = lax.axis_index("ep")
    core = lax.rem(me, 2)
    xpos = me // 2
    right = 2 * lax.rem(xpos + 1, 4) + core
    left = 2 * lax.rem(xpos + 3, 4) + core
    far = 2 * lax.rem(xpos + 2, 4) + core
    mate = 2 * xpos + 1 - core
    half = tok // 2
    rows = tok // 8

    def remote(src, dst, send, recv, dev):
        return pltpu.make_async_remote_copy(src_ref=src, dst_ref=dst, send_sem=send, recv_sem=recv, device_id={"ep": dev}, device_id_type=MESH)

    def local(src, dst, sem):
        return pltpu.make_async_copy(src, dst, sem)

    def o1(b, h):
        return acc.at[b, pl.ds(0, cw), pl.ds((1 + h) * ff, ff)]

    def o2(b, e):
        return acc.at[b, pl.ds(0, ff), pl.ds(e * cw, cw)]

    def load(k, b, s, ref):
        return local(s, ref.at[b], wsem.at[k, b])

    barrier = pltpu.get_barrier_semaphore()
    for d in range(1, 8):
        pl.semaphore_signal(barrier, inc=1, device_id={"ep": lax.rem(me + d, 8)}, device_id_type=MESH)

    shared_loads = [load(0, 1, s1, w1v), load(1, 1, s3, w3v), load(2, 1, s2, w2v)]
    first_loads = [load(0, 0, w1.at[0], w1v), load(1, 0, w3.at[0], w3v), load(2, 0, w2.at[0], w2v)]
    second_loads = [load(0, 1, w1.at[1], w1v), load(1, 1, w3.at[1], w3v), load(2, 1, w2.at[1], w2v)]
    own_loads = [local(x_loc, xt, lsem.at[0]), local(dy_loc, dyt, lsem.at[1])]
    for c in own_loads + shared_loads + first_loads:
        c.start()
    pl.semaphore_wait(barrier, 7)

    def block(ref, slot):
        return ref.at[pl.ds(pl.multiple_of(slot * tok, tok), tok), :]

    gates = []
    for d in range(1, 8):
        peer = lax.rem(me + d, 8)
        gates.append(remote(gt.at[peer], gall.at[me], gsend.at[d], grecv.at[me], peer))
        gates[-1].start()
    own_gate = local(gt.at[me], gall.at[me], lsem.at[2])
    own_gate.start()

    plan = [
        (me, 0, right), (me, 1, left), (me, 1, right), (me, 0, left), (me, None, mate), (left, 0, right), (right, 1, left),
        (left, 0, mate), (right, 1, mate), (left, 1, mate), (right, 0, mate), (far, 0, mate), (far, 1, mate),
    ]

    def message(k):
        slot, part, dev = plan[k]
        copies = []
        for a, (own, every) in enumerate(((x_loc, x_all), (dy_loc, dy_all))):
            first, size = (0, tok) if part is None else (part * half, half)
            dst = every.at[pl.ds(pl.multiple_of(slot * tok + first, half), size), :]
            src = own.at[pl.ds(first, size), :] if k < 5 else dst
            copies.append(remote(src, dst, ssem.at[k, a], rsem.at[k, a], dev))
        return copies

    def send(k):
        for c in message(k):
            c.start()

    def arrived(k):
        for c in message(k):
            c.wait_recv()

    for k in (4, 0, 1, 2, 3):
        send(k)

    def forward(cols, wb, ab, routed, gate_row, ab_out, before_sum):
        if routed:
            gate = jnp.transpose(jnp.broadcast_to(gate_row, (128, tok)))
            kept = gate < jnp.inf
            gate = jnp.where(kept, gate, 0.0)
            for n in range(dim // 128):
                s = slice(n * 128, (n + 1) * 128)
                zt[:, s] = (dyt[:, s].astype(F32) * gate).astype(BF16)
            wide = jnp.concatenate([kept] * (cw // 128), axis=1)
            dz = zt
        else:
            dz = dyt
        for n in range(ff // cw):
            s = slice(n * cw, (n + 1) * cw)
            a = dot(xt[...], w1v[wb, :, s], NN)
            b = dot(xt[...], w3v[wb, :, s], NN)
            if routed:
                a = jnp.where(wide, a, 0.0)
                b = jnp.where(wide, b, 0.0)
            a = a.astype(BF16).astype(F32)
            b = b.astype(BF16).astype(F32)
            g = dot(dz[...], w2v[wb, s, :], NT)
            sig = jax.nn.sigmoid(a)
            silu = a * sig
            hid = (silu * b).astype(BF16)
            da = (g * b * sig * (1.0 + a * (1.0 - sig))).astype(BF16)
            db = (g * silu).astype(BF16)
            dat[:, s] = da
            dbt[:, s] = db
            for kind, value in enumerate((hid, da, db)):
                value = jnp.transpose(value)
                for h in range(2):
                    act[ab, kind, s, pl.ds(cols[h], half)] = value[:, h * half:(h + 1) * half]
        before_sum()
        for n in range(dim // cw):
            s = slice(n * cw, (n + 1) * cw)
            r = dot(dat[...], w1v[wb, s, :], NT) + dot(dbt[...], w3v[wb, s, :], NT)
            if routed:
                acc[ab_out, :, s] += r.astype(BF16).astype(F32)
            else:
                acc[ab_out, :, s] = r

    for c in own_loads + shared_loads:
        c.wait()
    keep = [local(xt, block(x_all, me), lsem.at[0]), local(dyt, block(dy_all, me), lsem.at[1])]
    for c in keep:
        c.start()
    forward((0, half), 1, 1, False, None, 1, lambda: None)
    for c in second_loads:
        c.start()
    save = local(acc.at[1], rsh, lsem.at[3])
    save.start()

    def shared_grads(n, _):
        s = pl.ds(pl.multiple_of(n * cw, cw), cw)
        outs = [local(o1(0, 0), sw1.at[s, :], o1s.at[0, 0]), local(o1(0, 1), sw3.at[s, :], o1s.at[0, 1]), local(o2(0, 0), sw2.at[:, s], o2s.at[0, 0])]

        @pl.when(n > 0)
        def _():
            for c in outs:
                c.wait()
        o1(0, 0)[...] = jnp.transpose(dot(act[1, 1, :, 0:tok], xt[:, s], NN))
        o1(0, 1)[...] = jnp.transpose(dot(act[1, 2, :, 0:tok], xt[:, s], NN))
        o2(0, 0)[...] = dot(act[1, 0, :, 0:tok], dyt[:, s], NN)
        for c in outs:
            c.start()
        return 0

    lax.fori_loop(0, dim // cw, shared_grads, 0)
    local(o1(0, 0), sw1.at[pl.ds(0, cw), :], o1s.at[0, 0]).wait()
    local(o1(0, 1), sw3.at[pl.ds(0, cw), :], o1s.at[0, 1]).wait()
    local(o2(0, 0), sw2.at[:, pl.ds(0, cw)], o2s.at[0, 0]).wait()
    save.wait()
    for c in keep + first_loads + second_loads + [own_gate]:
        c.wait()
    for d in range(1, 8):
        peer = lax.rem(me + d, 8)
        remote(gt.at[peer], gall.at[peer], gsend.at[d], grecv.at[peer], peer).wait_recv()

    def phase1(to_left):
        if to_left:
            return remote(q_sum.at[1, pl.ds(0, half), :], from_r.at[pl.ds(0, half), :], r1s.at[0], r1r.at[0], left)
        return remote(q_sum.at[1, pl.ds(half, half), :], from_l.at[pl.ds(half, half), :], r1s.at[1], r1r.at[1], right)

    def phase2(k, to_left):
        if to_left:
            s = pl.ds(half + k * rows, rows)
            return remote(q_sum.at[3, s, :], opp.at[s, :], r2s.at[0, k], r2r.at[0, k], left)
        s = pl.ds(k * rows, rows)
        return remote(q_sum.at[3, s, :], opp.at[s, :], r2s.at[1, k], r2r.at[1, k], right)

    def phase3(k, to_left):
        if to_left:
            s = pl.ds(pl.multiple_of(half + k * rows, rows), rows)
            return remote(acc.at[0, s, :], from_r.at[s, :], r3s.at[0, k], r3r.at[0, k], left)
        s = pl.ds(pl.multiple_of(k * rows, rows), rows)
        return remote(acc.at[0, s, :], from_l.at[s, :], r3s.at[1, k], r3r.at[1, k], right)

    def partial(i):
        return remote(acc.at[0], pp.at[i], psend.at[i], precv.at[i], mate)

    def tile(j, _):
        i = j // 2
        t = lax.rem(j, 2)
        mine = jnp.where(t == 0, 1 - core, core)
        top = 2 * lax.rem(xpos + jnp.where(i == 0, 0, jnp.where(i == 1, 3, jnp.where(i == 2, 1, 2))), 4) + mine
        low = 2 * lax.rem(xpos + jnp.where(i == 0, 0, jnp.where(i == 1, 1, jnp.where(i == 2, 3, 2))), 4) + mine
        cols = (pl.multiple_of(top * tok, tok), pl.multiple_of(low * tok + half, half))

        @pl.when(j == 0)
        def _():
            arrived(4)

        @pl.when(j == 2)
        def _():
            arrived(0)
            send(5)
            send(7)
            arrived(1)
            send(6)
            send(8)
            arrived(7)
            arrived(8)

        @pl.when(j == 4)
        def _():
            arrived(2)
            send(9)
            arrived(3)
            send(10)
            arrived(9)
            arrived(10)

        @pl.when(j == 6)
        def _():
            arrived(5)
            send(11)
            arrived(6)
            send(12)
            arrived(11)
            arrived(12)

        loads = [local(every.at[pl.ds(cols[h], half), :], buf.at[pl.ds(h * half, half), :], wsem.at[h, a])
                 for h in range(2) for a, (every, buf) in enumerate(((x_all, xt), (dy_all, dyt)))]
        for c in loads:
            c.start()
        for c in loads:
            c.wait()

        def expert(e, _):
            put_z = [local(zt.at[pl.ds(h * half, half), :], z_all.at[e, pl.ds(cols[h], half), :], lsem.at[1 + h]) for h in range(2)]

            def before_sum():
                for c in put_z:
                    c.start()

                @pl.when((e == 0) & (t == 0))
                def _():
                    @pl.when(i > 0)
                    def _():
                        partial(i - 1).wait_send()
                    acc[0] = jnp.zeros((tok, dim), F32)

                @pl.when((e == 0) & (t == 1))
                def _():
                    partial(i).wait_recv()
                    get = local(pp.at[i], acc.at[1], lsem.at[3])
                    get.start()
                    get.wait()

            gate_row = jnp.concatenate([gall[top, pl.ds(e, 1), 0:half], gall[low, pl.ds(e, 1), half:tok]], axis=1)
            forward(cols, e, e, True, gate_row, t, before_sum)
            for c in put_z:
                c.wait()
            return 0

        lax.fori_loop(0, 2, expert, 0)

        @pl.when(t == 0)
        def _():
            partial(i).start()

        @pl.when(t == 1)
        def _():
            put = local(acc.at[1], q_sum.at[i], lsem.at[3])
            put.start()
            put.wait()

        @pl.when(j == 3)
        def _():
            phase1(True).start()
            phase1(False).start()

        @pl.when(j == 7)
        def _():
            for k in range(4):
                phase2(k, True).start()
                phase2(k, False).start()
        return 0

    lax.fori_loop(0, 8, tile, 0)
    partial(3).wait_send()

    def combine(k):
        for to_left in (False, True):
            base = half if to_left else 0
            s = pl.ds(pl.multiple_of(base + k * rows, rows), rows)
            b = 0 if to_left else 1
            remote(opp.at[s, :], opp.at[s, :], r2s.at[b, k], r2r.at[b, k], right).wait_recv()
            gets = [local(opp.at[s, :], acc.at[0, s, :], lsem.at[0]), local(q_sum.at[2, s, :], tmp.at[0], lsem.at[1])]
            for c in gets:
                c.start()
            for c in gets:
                c.wait()
            acc[0, s, :] += tmp[0]
            phase3(k, to_left).start()

    chunks = dim // cw

    def column(n):
        return pl.ds(pl.multiple_of(n * cw, cw), cw)

    deep = 4 * tok

    def fetch(n, b):
        whole = [local(x_all.at[:, column(n)], xc.at[b], xcs.at[b])]
        for e, buf in ((0, w1v), (1, w3v)):
            for h in range(2):
                whole.append(local(z_all.at[e, pl.ds(h * deep, deep), column(n)], buf.at[b, pl.ds(0, deep), pl.ds(h * cw, cw)], zcs.at[e, h, b]))
        return whole

    def stage(e, kind, h):
        if kind < 2:
            return acc.at[1, pl.ds(0, cw), pl.ds((2 * e + kind) * ff, ff)]
        return acc.at[1, pl.ds(cw, ff // 2), pl.ds((2 * e + h) * cw, cw)]

    def results(n):
        puts = []
        for e in range(2):
            puts.append(local(stage(e, 0, 0), dw1.at[e, column(n), :], o1s.at[e, 0]))
            puts.append(local(stage(e, 1, 0), dw3.at[e, column(n), :], o1s.at[e, 1]))
            for h in range(2):
                puts.append(local(stage(e, 2, h), dw2.at[e, pl.ds(h * (ff // 2), ff // 2), column(n)], o2s.at[e, h]))
        return puts

    for c in fetch(0, 0):
        c.start()

    def weight_grads(n, _):
        b = lax.rem(n, 2)
        for c in fetch(n, b):
            c.wait()

        @pl.when(n > 0)
        def _():
            for c in results(n - 1):
                c.wait()

        @pl.when(n < chunks - 1)
        def _():
            for c in fetch(n + 1, 1 - b):
                c.start()
        for e, buf in ((0, w1v), (1, w3v)):
            for kind in range(2):
                stage(e, kind, 0)[...] = jnp.transpose(dot(act[e, 1 + kind], xc[b], NN))
            for h in range(2):
                f = slice(h * (ff // 2), (h + 1) * (ff // 2))
                stage(e, 2, h)[...] = dot(act[e, 0, f, 0:deep], buf[b, 0:deep, 0:cw], NN) + dot(act[e, 0, f, deep:2 * deep], buf[b, 0:deep, cw:2 * cw], NN)
        for c in results(n):
            c.start()

        @pl.when(n >= chunks - 4)
        def _():
            combine(n - (chunks - 4))
        return 0

    lax.fori_loop(0, chunks, weight_grads, 0)
    for c in results(chunks - 1):
        c.wait()

    get = local(q_sum.at[0], acc.at[1], lsem.at[2])
    get.start()
    phase1(True).wait_recv()
    phase1(False).wait_recv()
    get.wait()

    def own_rows(k, _):
        s = pl.ds(pl.multiple_of(k * rows, rows), rows)
        first = local(rsh.at[s, :], tmp.at[0], lsem.at[0])
        first.start()

        @pl.when(k < 4)
        def _():
            local(from_r.at[s, :], tmp.at[1], lsem.at[1]).start()

        @pl.when(k >= 4)
        def _():
            local(from_l.at[s, :], tmp.at[1], lsem.at[1]).start()
        first.wait()
        local(from_l.at[s, :], tmp.at[1], lsem.at[1]).wait()
        acc[1, s, :] += tmp[0] + tmp[1]
        return 0

    lax.fori_loop(0, 8, own_rows, 0)

    def last(k):
        sa, sb = pl.ds(k * rows, rows), pl.ds(half + k * rows, rows)
        phase3(k, False).wait_recv()
        ga = local(from_l.at[sa, :], tmp.at[0], lsem.at[0])
        ga.start()
        phase3(k, True).wait_recv()
        gb = local(from_r.at[sb, :], tmp.at[1], lsem.at[1])
        gb.start()
        ga.wait()
        xt[sa, :] = (acc[1, sa, :] + tmp[0]).astype(BF16)
        pa = local(xt.at[sa, :], gx.at[sa, :], gxs.at[0, k])
        pa.start()
        gb.wait()
        xt[sb, :] = (acc[1, sb, :] + tmp[1]).astype(BF16)
        pb = local(xt.at[sb, :], gx.at[sb, :], gxs.at[1, k])
        pb.start()
        return [pa, pb]

    puts = []
    for k in range(4):
        puts += last(k)
    for c in puts:
        c.wait()
    for c in gates:
        c.wait_send()
    for k in range(13):
        for c in message(k):
            c.wait_send()
    for to_left in (True, False):
        phase1(to_left).wait_send()
        for k in range(4):
            phase2(k, to_left).wait_send()
            phase3(k, to_left).wait_send()


def moe_call(x, dy, gt, w1, w3, w2, s1, s3, s2):
    tok, dim = x.shape
    ff = w1.shape[2]
    cw = CW
    sds = jax.ShapeDtypeStruct
    outs = [
        sds((tok, dim), BF16), sds((2, dim, ff), F32), sds((2, dim, ff), F32), sds((2, ff, dim), F32),
        sds((dim, ff), F32), sds((dim, ff), F32), sds((ff, dim), F32),
        sds((8 * tok, dim), BF16), sds((8 * tok, dim), BF16), sds((2, 8 * tok, dim), BF16),
        sds((4, tok, dim), F32), sds((4, tok, dim), F32), sds((tok, dim), F32), sds((tok, dim), F32), sds((tok, dim), F32), sds((tok, dim), F32),
    ]
    V, D = pltpu.VMEM, pltpu.SemaphoreType.DMA
    scratch = [
        V((2, dim, ff), BF16), V((2, dim, ff), BF16), V((2, ff, dim), BF16), V((2, 3, ff, 8 * tok), BF16),
        V((tok, dim), BF16), V((tok, dim), BF16), V((tok, dim), BF16), V((tok, ff), BF16), V((tok, ff), BF16),
        V((2, tok, dim), F32), V((2, 8 * tok, cw), BF16), V((2, tok // 8, dim), F32),
        V((8, 8, tok), F32),
        D((3, 2)), D((8,)), D((8,)), D((13, 2)), D((13, 2)), D((4,)), D((4,)), D((2,)), D((2,)),
        D((2, 4)), D((2, 4)), D((2, 4)), D((2, 4)), D((4,)), D((2,)), D((2, 2, 2)), D((2, 2)), D((2, 2)), D((2, 4)),
    ]
    any_spec = pl.BlockSpec(memory_space=pl.ANY)
    return pl.pallas_call(
        functools.partial(moe_kernel, tok, dim, ff, cw),
        out_shape=outs,
        in_specs=[any_spec] * 9,
        out_specs=[any_spec] * len(outs),
        scratch_shapes=scratch,
        compiler_params=pltpu.CompilerParams(collective_id=0, has_side_effects=True, vmem_limit_bytes=67043328),
        name="moe_backward",
    )(x, dy, gt, w1, w3, w2, s1, s3, s2)[:7]


def solution(mesh):
    group = mesh.shape['ep']
    token_spec = P(('dp', 'ep'), None)
    expert_spec = P('ep', None, None)
    whole_spec = P(None, None)
    grad_spec = P(('dp', 'ep'), None, None)

    def local_backward(x_tokens, dy_tokens, expert_ids, gate_vals, slot_pos, w_gate, w_up, w_down, shared_gate, shared_up, shared_down):
        tok_count, top_k = expert_ids.shape
        num_experts = w_gate.shape[0] * group
        ids, pos, gates = expert_ids.T, slot_pos.T, gate_vals.T
        experts = jnp.arange(num_experts, dtype=jnp.int32)[:, None]
        table = jnp.full((num_experts, tok_count), jnp.inf, F32)
        for j in range(top_k):
            table = jnp.where((ids[j:j + 1] == experts) & (pos[j:j + 1] >= 0), gates[j:j + 1], table)
        table = jnp.pad(table.reshape(group, -1, tok_count), ((0, 0), (0, 8 - num_experts // group), (0, 0)))
        gx, dw1, dw3, dw2, sw1, sw3, sw2 = moe_call(x_tokens, dy_tokens, table, w_gate, w_up, w_down, shared_gate, shared_up, shared_down)
        return gx, dw1, dw3, dw2, sw1[None], sw3[None], sw2[None]

    return jax.shard_map(local_backward, mesh=mesh, in_specs=(token_spec, token_spec, token_spec, token_spec, token_spec, expert_spec, expert_spec, expert_spec, whole_spec, whole_spec, whole_spec), out_specs=(token_spec, grad_spec, grad_spec, grad_spec, grad_spec, grad_spec, grad_spec), check_vma=False)
```

```python
import functools

import jax
import jax.numpy as jnp
from jax import lax
from jax.experimental import pallas as pl
from jax.experimental.pallas import tpu as pltpu
from jax.sharding import PartitionSpec as P

CW = 256
SENT = 2
F32, BF16 = jnp.float32, jnp.bfloat16
MESH = pl.DeviceIdType.MESH
NN = (((1,), (0,)), ((), ()))
NT = (((1,), (1,)), ((), ()))


def dot(a, b, dims):
    return lax.dot_general(a, b, dims, preferred_element_type=F32)


def moe_kernel(tok, dim, ff, cw, x_loc, dy_loc, gt, w1, w3, w2, s1, s3, s2,
               dw1, dw3, dw2, sw1, sw3, sw2, x_all, dy_all, z_all, pp, q_sum, rsh, from_l, from_r, late_a, late_b, opp,
               w1v, w3v, w2v, act, xt, dyt, zt, dat, dbt, acc, xc, tmp, gall,
               wsem, gsend, grecv, ssem, rsem, psend, precv, r1s, r1r, r2s, r2r, r3s, r3r, lsem, xcs, zcs, o1s, o2s, cs, ms):
    me = lax.axis_index("ep")
    core = lax.rem(me, 2)
    xpos = me // 2
    right = 2 * lax.rem(xpos + 1, 4) + core
    left = 2 * lax.rem(xpos + 3, 4) + core
    far = 2 * lax.rem(xpos + 2, 4) + core
    mate = 2 * xpos + 1 - core
    half = tok // 2
    rows = tok // 8

    def remote(src, dst, send, recv, dev):
        return pltpu.make_async_remote_copy(src_ref=src, dst_ref=dst, send_sem=send, recv_sem=recv, device_id={"ep": dev}, device_id_type=MESH)

    def local(src, dst, sem):
        return pltpu.make_async_copy(src, dst, sem)

    def o1(b, h):
        return acc.at[b, pl.ds(0, cw), pl.ds((1 + h) * ff, ff)]

    def o2(b, e):
        return acc.at[b, pl.ds(0, ff), pl.ds(e * cw, cw)]

    def load(k, b, s, ref):
        return local(s, ref.at[b], wsem.at[k, b])

    barrier = pltpu.get_barrier_semaphore()
    for d in range(1, 8):
        pl.semaphore_signal(barrier, inc=1, device_id={"ep": lax.rem(me + d, 8)}, device_id_type=MESH)

    shared_loads = [load(0, 1, s1, w1v), load(1, 1, s3, w3v), load(2, 1, s2, w2v)]
    first_loads = [load(0, 0, w1.at[0], w1v), load(1, 0, w3.at[0], w3v), load(2, 0, w2.at[0], w2v)]
    second_loads = [load(0, 1, w1.at[1], w1v), load(1, 1, w3.at[1], w3v), load(2, 1, w2.at[1], w2v)]
    own_loads = [local(x_loc, xt, lsem.at[0]), local(dy_loc, dyt, lsem.at[1])]
    for c in own_loads + shared_loads + first_loads:
        c.start()
    pl.semaphore_wait(barrier, 7)

    def block(ref, slot):
        return ref.at[pl.ds(pl.multiple_of(slot * tok, tok), tok), :]

    gates = []
    for d in range(1, 8):
        peer = lax.rem(me + d, 8)
        gates.append(remote(gt.at[peer], gall.at[me], gsend.at[d], grecv.at[me], peer))
        gates[-1].start()
    own_gate = local(gt.at[me], gall.at[me], lsem.at[2])
    own_gate.start()

    plan = [
        (me, 0, right), (me, 1, left), (me, 1, right), (me, 0, left), (me, None, mate), (left, 0, right), (right, 1, left),
        (left, 0, mate), (right, 1, mate), (left, 1, mate), (right, 0, mate), (far, 0, mate), (far, 1, mate),
    ]

    def message(k):
        slot, part, dev = plan[k]
        copies = []
        for a, (own, every) in enumerate(((x_loc, x_all), (dy_loc, dy_all))):
            first, size = (0, tok) if part is None else (part * half, half)
            dst = every.at[pl.ds(pl.multiple_of(slot * tok + first, half), size), :]
            src = own.at[pl.ds(first, size), :] if k < 5 else dst
            copies.append(remote(src, dst, ssem.at[k, a], rsem.at[k, a], dev))
        return copies

    def send(k):
        for c in message(k):
            c.start()

    def arrived(k):
        for c in message(k):
            c.wait_recv()

    for k in (4, 0, 1, 2, 3):
        send(k)

    def forward(cols, wb, ab, routed, gate_row, ab_out, before_sum):
        if routed:
            gate = jnp.transpose(jnp.broadcast_to(gate_row, (128, tok)))
            kept = gate < jnp.inf
            gate = jnp.where(kept, gate, 0.0)
            for n in range(dim // 128):
                s = slice(n * 128, (n + 1) * 128)
                zt[:, s] = (dyt[:, s].astype(F32) * gate).astype(BF16)
            wide = jnp.concatenate([kept] * (cw // 128), axis=1)
            dz = zt
        else:
            dz = dyt
        for n in range(ff // cw):
            s = slice(n * cw, (n + 1) * cw)
            a = dot(xt[...], w1v[wb, :, s], NN)
            b = dot(xt[...], w3v[wb, :, s], NN)
            if routed:
                a = jnp.where(wide, a, 0.0)
                b = jnp.where(wide, b, 0.0)
            a = a.astype(BF16).astype(F32)
            b = b.astype(BF16).astype(F32)
            g = dot(dz[...], w2v[wb, s, :], NT)
            sig = jax.nn.sigmoid(a)
            silu = a * sig
            hid = (silu * b).astype(BF16)
            da = (g * b * sig * (1.0 + a * (1.0 - sig))).astype(BF16)
            db = (g * silu).astype(BF16)
            dat[:, s] = da
            dbt[:, s] = db
            for kind, value in enumerate((hid, da, db)):
                value = jnp.transpose(value)
                for h in range(2):
                    act[ab, kind, s, pl.ds(cols[h], half)] = value[:, h * half:(h + 1) * half]
        before_sum()
        for n in range(dim // cw):
            s = slice(n * cw, (n + 1) * cw)
            r = dot(dat[...], w1v[wb, s, :], NT) + dot(dbt[...], w3v[wb, s, :], NT)
            if routed:
                acc[ab_out, :, s] += r.astype(BF16).astype(F32)
            else:
                acc[ab_out, :, s] = r

    for c in own_loads + shared_loads:
        c.wait()
    keep = [local(xt, block(x_all, me), lsem.at[0]), local(dyt, block(dy_all, me), lsem.at[1])]
    for c in keep:
        c.start()
    forward((0, half), 1, 1, False, None, 1, lambda: None)
    for c in second_loads:
        c.start()
    save = local(acc.at[1], rsh, lsem.at[3])
    save.start()

    def shared_grads(n, _):
        s = pl.ds(pl.multiple_of(n * cw, cw), cw)
        outs = [local(o1(0, 0), sw1.at[s, :], o1s.at[0, 0]), local(o1(0, 1), sw3.at[s, :], o1s.at[0, 1]), local(o2(0, 0), sw2.at[:, s], o2s.at[0, 0])]

        @pl.when(n > 0)
        def _():
            for c in outs:
                c.wait()
        o1(0, 0)[...] = jnp.transpose(dot(act[1, 1, :, 0:tok], xt[:, s], NN))
        o1(0, 1)[...] = jnp.transpose(dot(act[1, 2, :, 0:tok], xt[:, s], NN))
        o2(0, 0)[...] = dot(act[1, 0, :, 0:tok], dyt[:, s], NN)
        for c in outs:
            c.start()
        return 0

    lax.fori_loop(0, dim // cw, shared_grads, 0)
    local(o1(0, 0), sw1.at[pl.ds(0, cw), :], o1s.at[0, 0]).wait()
    local(o1(0, 1), sw3.at[pl.ds(0, cw), :], o1s.at[0, 1]).wait()
    local(o2(0, 0), sw2.at[:, pl.ds(0, cw)], o2s.at[0, 0]).wait()
    save.wait()
    for c in keep + first_loads + second_loads + [own_gate]:
        c.wait()
    for d in range(1, 8):
        peer = lax.rem(me + d, 8)
        remote(gt.at[peer], gall.at[peer], gsend.at[d], grecv.at[peer], peer).wait_recv()

    def phase1(to_left):
        if to_left:
            return remote(q_sum.at[1, pl.ds(0, half), :], from_r.at[pl.ds(0, half), :], r1s.at[0], r1r.at[0], left)
        return remote(q_sum.at[1, pl.ds(half, half), :], from_l.at[pl.ds(half, half), :], r1s.at[1], r1r.at[1], right)

    def phase2(k, to_left):
        if to_left:
            s = pl.ds(half + k * rows, rows)
            return remote(q_sum.at[3, s, :], opp.at[s, :], r2s.at[0, k], r2r.at[0, k], left)
        s = pl.ds(k * rows, rows)
        return remote(q_sum.at[3, s, :], opp.at[s, :], r2s.at[1, k], r2r.at[1, k], right)

    def phase3(k, to_left):
        if to_left:
            s = pl.ds(pl.multiple_of(half + k * rows, rows), rows)
            return remote(acc.at[0, s, :], from_r.at[s, :], r3s.at[0, k], r3r.at[0, k], left)
        s = pl.ds(pl.multiple_of(k * rows, rows), rows)
        return remote(acc.at[0, s, :], from_l.at[s, :], r3s.at[1, k], r3r.at[1, k], right)

    def partial(i):
        return remote(acc.at[0], pp.at[i], psend.at[i], precv.at[i], mate)

    def tile(j, _):
        i = j // 2
        t = lax.rem(j, 2)
        mine = jnp.where(t == 0, 1 - core, core)
        top = 2 * lax.rem(xpos + jnp.where(i == 0, 0, jnp.where(i == 1, 3, jnp.where(i == 2, 1, 2))), 4) + mine
        low = 2 * lax.rem(xpos + jnp.where(i == 0, 0, jnp.where(i == 1, 1, jnp.where(i == 2, 3, 2))), 4) + mine
        cols = (pl.multiple_of(top * tok, tok), pl.multiple_of(low * tok + half, half))

        @pl.when(j == 0)
        def _():
            arrived(4)

        @pl.when(j == 2)
        def _():
            arrived(0)
            send(5)
            send(7)
            arrived(1)
            send(6)
            send(8)
            arrived(7)
            arrived(8)

        @pl.when(j == 4)
        def _():
            arrived(2)
            send(9)
            arrived(3)
            send(10)
            arrived(9)
            arrived(10)

        @pl.when(j == 6)
        def _():
            arrived(5)
            send(11)
            arrived(6)
            send(12)
            arrived(11)
            arrived(12)

        loads = [local(every.at[pl.ds(cols[h], half), :], buf.at[pl.ds(h * half, half), :], wsem.at[h, a])
                 for h in range(2) for a, (every, buf) in enumerate(((x_all, xt), (dy_all, dyt)))]
        for c in loads:
            c.start()
        for c in loads:
            c.wait()

        def expert(e, _):
            put_z = [local(zt.at[pl.ds(h * half, half), :], z_all.at[e, pl.ds(cols[h], half), :], lsem.at[1 + h]) for h in range(2)]

            def before_sum():
                for c in put_z:
                    c.start()

                @pl.when((e == 0) & (t == 0))
                def _():
                    @pl.when(i > 0)
                    def _():
                        partial(i - 1).wait_send()
                    acc[0] = jnp.zeros((tok, dim), F32)

                @pl.when((e == 0) & (t == 1))
                def _():
                    partial(i).wait_recv()
                    get = local(pp.at[i], acc.at[1], lsem.at[3])
                    get.start()
                    get.wait()

            gate_row = jnp.concatenate([gall[top, pl.ds(e, 1), 0:half], gall[low, pl.ds(e, 1), half:tok]], axis=1)
            forward(cols, e, e, True, gate_row, t, before_sum)
            for c in put_z:
                c.wait()
            return 0

        lax.fori_loop(0, 2, expert, 0)

        @pl.when(t == 0)
        def _():
            partial(i).start()

        @pl.when(t == 1)
        def _():
            put = local(acc.at[1], q_sum.at[i], lsem.at[3])
            put.start()
            put.wait()

        @pl.when(j == 3)
        def _():
            phase1(True).start()
            phase1(False).start()

        @pl.when(j == 7)
        def _():
            for k in range(4):
                phase2(k, True).start()
                phase2(k, False).start()
        return 0

    lax.fori_loop(0, 8, tile, 0)
    partial(3).wait_send()

    def kept_sum(k, to_left):
        s = pl.ds(pl.multiple_of((half if to_left else 0) + k * rows, rows), rows)
        return local(acc.at[0, s, :], (late_b if to_left else late_a).at[pl.ds(pl.multiple_of((k - SENT) * rows, rows), rows), :], cs.at[1 if to_left else 0, k])

    def operands(k):
        gets = []
        for b, base in ((1, 0), (0, half)):
            s = pl.ds(pl.multiple_of(base + k * rows, rows), rows)
            gets.append(local(opp.at[s, :], acc.at[0, s, :], ms.at[b, 0]))
            gets.append(local(q_sum.at[2, s, :], tmp.at[b], ms.at[b, 1]))
        return gets

    def begin_combine(k):
        for b, base in ((1, 0), (0, half)):
            s = pl.ds(pl.multiple_of(base + k * rows, rows), rows)
            remote(opp.at[s, :], opp.at[s, :], r2s.at[b, k], r2r.at[b, k], right).wait_recv()
        for c in operands(k):
            c.start()

    def combine(k):
        for c in operands(k):
            c.wait()
        for to_left in (False, True):
            s = pl.ds(pl.multiple_of((half if to_left else 0) + k * rows, rows), rows)
            acc[0, s, :] += tmp[0 if to_left else 1]

            @pl.when(k < SENT)
            def _():
                phase3(k, to_left).start()

            @pl.when(k >= SENT)
            def _():
                kept_sum(k, to_left).start()

    chunks = dim // cw

    def column(n):
        return pl.ds(pl.multiple_of(n * cw, cw), cw)

    deep = 4 * tok

    def fetch(n, b):
        whole = [local(x_all.at[:, column(n)], xc.at[b], xcs.at[b])]
        for e, buf in ((0, w1v), (1, w3v)):
            for h in range(2):
                whole.append(local(z_all.at[e, pl.ds(h * deep, deep), column(n)], buf.at[b, pl.ds(0, deep), pl.ds(h * cw, cw)], zcs.at[e, h, b]))
        return whole

    def stage(e, kind, h):
        if kind < 2:
            return acc.at[1, pl.ds(0, cw), pl.ds((2 * e + kind) * ff, ff)]
        return acc.at[1, pl.ds(cw, ff // 2), pl.ds((2 * e + h) * cw, cw)]

    def results(n):
        puts = []
        for e in range(2):
            puts.append(local(stage(e, 0, 0), dw1.at[e, column(n), :], o1s.at[e, 0]))
            puts.append(local(stage(e, 1, 0), dw3.at[e, column(n), :], o1s.at[e, 1]))
            for h in range(2):
                puts.append(local(stage(e, 2, h), dw2.at[e, pl.ds(h * (ff // 2), ff // 2), column(n)], o2s.at[e, h]))
        return puts

    for c in fetch(0, 0):
        c.start()

    def weight_grads(n, _):
        b = lax.rem(n, 2)
        for c in fetch(n, b):
            c.wait()

        @pl.when(n > 0)
        def _():
            for c in results(n - 1):
                c.wait()

        @pl.when(n < chunks - 1)
        def _():
            for c in fetch(n + 1, 1 - b):
                c.start()

        @pl.when(n >= chunks - 4)
        def _():
            begin_combine(n - (chunks - 4))
        for e, buf in ((0, w1v), (1, w3v)):
            for kind in range(2):
                stage(e, kind, 0)[...] = jnp.transpose(dot(act[e, 1 + kind], xc[b], NN))
            for h in range(2):
                f = slice(h * (ff // 2), (h + 1) * (ff // 2))
                stage(e, 2, h)[...] = dot(act[e, 0, f, 0:deep], buf[b, 0:deep, 0:cw], NN) + dot(act[e, 0, f, deep:2 * deep], buf[b, 0:deep, cw:2 * cw], NN)
        for c in results(n):
            c.start()

        @pl.when(n >= chunks - 4)
        def _():
            combine(n - (chunks - 4))
        return 0

    lax.fori_loop(0, chunks, weight_grads, 0)
    for c in results(chunks - 1):
        c.wait()

    phase1(True).wait_recv()
    phase1(False).wait_recv()
    for to_left in (True, False):
        for k in range(SENT):
            phase3(k, to_left).wait_recv()
        for k in range(SENT, 4):
            kept_sum(k, to_left).wait()
    for c in gates:
        c.wait_send()
    for k in range(13):
        for c in message(k):
            c.wait_send()
    for to_left in (True, False):
        phase1(to_left).wait_send()
        for k in range(4):
            phase2(k, to_left).wait_send()
        for k in range(SENT):
            phase3(k, to_left).wait_send()


def moe_call(x, dy, gt, w1, w3, w2, s1, s3, s2):
    tok, dim = x.shape
    ff = w1.shape[2]
    cw = CW
    sds = jax.ShapeDtypeStruct
    outs = [
        sds((2, dim, ff), F32), sds((2, dim, ff), F32), sds((2, ff, dim), F32),
        sds((dim, ff), F32), sds((dim, ff), F32), sds((ff, dim), F32),
        sds((8 * tok, dim), BF16), sds((8 * tok, dim), BF16), sds((2, 8 * tok, dim), BF16),
        sds((4, tok, dim), F32), sds((4, tok, dim), F32), sds((tok, dim), F32), sds((tok, dim), F32), sds((tok, dim), F32),
        sds(((4 - SENT) * (tok // 8), dim), F32), sds(((4 - SENT) * (tok // 8), dim), F32), sds((tok, dim), F32),
    ]
    V, D = pltpu.VMEM, pltpu.SemaphoreType.DMA
    scratch = [
        V((2, dim, ff), BF16), V((2, dim, ff), BF16), V((2, ff, dim), BF16), V((2, 3, ff, 8 * tok), BF16),
        V((tok, dim), BF16), V((tok, dim), BF16), V((tok, dim), BF16), V((tok, ff), BF16), V((tok, ff), BF16),
        V((2, tok, dim), F32), V((2, 8 * tok, cw), BF16), V((2, tok // 8, dim), F32),
        V((8, 8, tok), F32),
        D((3, 2)), D((8,)), D((8,)), D((13, 2)), D((13, 2)), D((4,)), D((4,)), D((2,)), D((2,)),
        D((2, 4)), D((2, 4)), D((2, 4)), D((2, 4)), D((4,)), D((2,)), D((2, 2, 2)), D((2, 2)), D((2, 2)), D((2, 4)), D((2, 2)),
    ]
    any_spec = pl.BlockSpec(memory_space=pl.ANY)
    return pl.pallas_call(
        functools.partial(moe_kernel, tok, dim, ff, cw),
        out_shape=outs,
        in_specs=[any_spec] * 9,
        out_specs=[any_spec] * len(outs),
        scratch_shapes=scratch,
        compiler_params=pltpu.CompilerParams(collective_id=0, has_side_effects=True, vmem_limit_bytes=67043328),
        name="moe_backward",
    )(x, dy, gt, w1, w3, w2, s1, s3, s2)


def put_kernel(q, rsh, from_l, from_r, *refs):
    count = (len(refs) - 1) // 2
    for src, dst in zip(refs[:count], refs[count + 1:]):
        dst[...] = src[...]
    base = refs[count]
    step, steps = pl.program_id(0), pl.num_programs(0)
    both = lax.rem(step, steps // 2) < SENT * steps // 8
    own = q[0] + rsh[...]

    @pl.when(both)
    def _():
        base[...] = own + (from_l[...] + from_r[...])

    @pl.when(jnp.logical_not(both) & (step < steps // 2))
    def _():
        base[...] = own + from_r[...]

    @pl.when(jnp.logical_not(both) & (step >= steps // 2))
    def _():
        base[...] = own + from_l[...]


def put_out(q_sum, rsh, from_l, from_r, *arrays):
    steps = 8
    tok, dim = rsh.shape

    def spec(a):
        shape = a.shape[:-2] + (a.shape[-2] // steps, a.shape[-1])
        lead = (0,) * (a.ndim - 2)
        return pl.BlockSpec(shape, lambda i: lead + (i, 0))

    size = sum(a.size * a.dtype.itemsize for a in arrays)
    specs = [spec(a) for a in arrays]
    row = pl.BlockSpec((tok // steps, dim), lambda i: (i, 0))
    return pl.pallas_call(
        put_kernel, grid=(steps,),
        in_specs=[pl.BlockSpec((1, tok // steps, dim), lambda i: (0, i, 0)), row, row, row] + specs,
        out_specs=[row] + specs,
        out_shape=[jax.ShapeDtypeStruct((tok, dim), F32)] + [jax.ShapeDtypeStruct(a.shape, a.dtype) for a in arrays],
        compiler_params=pltpu.CompilerParams(vmem_limit_bytes=67043328),
        cost_estimate=pl.CostEstimate(flops=size * 1000, bytes_accessed=2 * size, transcendentals=0),
        name="put_out",
    )(q_sum, rsh, from_l, from_r, *arrays)


def last_kernel(base, late_l, late_r, out):
    done = SENT * base.shape[0] // 4
    out[:done] = base[:done].astype(BF16)

    @pl.when(pl.program_id(0) == 0)
    def _():
        out[done:] = (base[done:] + late_l[...]).astype(BF16)

    @pl.when(pl.program_id(0) == 1)
    def _():
        out[done:] = (base[done:] + late_r[...]).astype(BF16)


def last_sum(base, late_l, late_r):
    tok, dim = base.shape
    row = pl.BlockSpec((tok // 2, dim), lambda i: (i, 0))
    late = pl.BlockSpec(late_l.shape, lambda i: (0, 0))
    return pl.pallas_call(
        last_kernel, grid=(2,), in_specs=[row, late, late], out_specs=row,
        out_shape=jax.ShapeDtypeStruct((tok, dim), BF16),
        compiler_params=pltpu.CompilerParams(vmem_limit_bytes=67043328),
        name="last_sum",
    )(base, late_l, late_r)


def solution(mesh):
    group = mesh.shape['ep']
    token_spec = P(('dp', 'ep'), None)
    expert_spec = P('ep', None, None)
    whole_spec = P(None, None)
    grad_spec = P(('dp', 'ep'), None, None)

    def local_backward(x_tokens, dy_tokens, expert_ids, gate_vals, slot_pos, w_gate, w_up, w_down, shared_gate, shared_up, shared_down):
        tok_count, top_k = expert_ids.shape
        num_experts = w_gate.shape[0] * group
        ids, pos, gates = expert_ids.T, slot_pos.T, gate_vals.T
        experts = jnp.arange(num_experts, dtype=jnp.int32)[:, None]
        table = jnp.full((num_experts, tok_count), jnp.inf, F32)
        for j in range(top_k):
            table = jnp.where((ids[j:j + 1] == experts) & (pos[j:j + 1] >= 0), gates[j:j + 1], table)
        table = jnp.pad(table.reshape(group, -1, tok_count), ((0, 0), (0, 8 - num_experts // group), (0, 0)))
        dw1, dw3, dw2, sw1, sw3, sw2, _, _, _, _, q_sum, rsh, from_l, from_r, late_a, late_b, _ = moe_call(x_tokens, dy_tokens, table, w_gate, w_up, w_down, shared_gate, shared_up, shared_down)
        ring = [2 * ((i // 2 + 1) % (group // 2)) + i % 2 for i in range(group)]
        late_l = lax.ppermute(late_a, 'ep', [(i, r) for i, r in enumerate(ring)])
        late_r = lax.ppermute(late_b, 'ep', [(r, i) for i, r in enumerate(ring)])
        base, dw1, dw3, dw2, sw1, sw3, sw2 = put_out(q_sum, rsh, from_l, from_r, dw1, dw3, dw2, sw1, sw3, sw2)
        gx = last_sum(base, late_l, late_r)
        return gx, dw1, dw3, dw2, sw1[None], sw3[None], sw2[None]

    return jax.shard_map(local_backward, mesh=mesh, in_specs=(token_spec, token_spec, token_spec, token_spec, token_spec, expert_spec, expert_spec, expert_spec, whole_spec, whole_spec, whole_spec), out_specs=(token_spec, grad_spec, grad_spec, grad_spec, grad_spec, grad_spec, grad_spec), check_vma=False)
```
